32 devices in a mesh: groups: 2 (over x), tok: 16 (over z, y, core).
Axes of the slice: x: 2, y: 2, z: 4, core: 2. Of those that a mesh axis runs over, the one named last changes fastest.
Arguments:
- activations: bfloat16 [8, 4096, 128], P(None, ('groups', 'tok')), parts along dimension 1, may hold values from -1.796875 to 1.796875
- gradients: bfloat16 [8, 4096, 128], P(None, ('groups', 'tok')), parts along dimension 1, may hold values from -1.796875 to 1.796875
- queries: bfloat16 [64, 4096], P(None, ('groups', 'tok')), parts along dimension 1, may hold values from -0.125 to 0.125
- layer_ids: int32 [3], replicated, may hold values from 0 to 7
Outputs:
- influence: float32 [64, 4096], P(None, ('groups', 'tok')), parts along dimension 1
The draws below stay inside these ranges and needn't reach their ends.
There are 2 independent parts, one for each index of `groups`. The reference program is written for one: setup_inputs(seed, part) draws one part's arguments, and reference() takes and returns one part's arrays. A program takes and returns all parts, laid end to end along the dimension named above; an argument that names none is the same for every part. Nothing has to cross between parts.
Inputs may be any that keep to these rules, and one draw needn't show every extreme that they name: `layer_ids`: indices of stored layers; they may repeat.
All inputs are finite; a program needn't handle non-finite values.
Results may differ from the reference program's by a relative error of at most 0.0029.
Values may be sent and summed in bfloat16 or wider, within the bound.
No kernel may reach another device: no remote copies, remote signals or barrier semaphores. Data moves between devices by JAX's collectives and lax.ppermute only.
A program may use at most 64 MiB of HBM per device.

```python
import math
import jax
import jax.numpy as jnp
from jax import lax

R = 128
Q = 64
NL = 8
LS = 3
TOKENS = 2048


def level_of(stream_key, extent, cuts, least, high):
    def one(position, parts):
        heights = jax.random.uniform(jax.random.fold_in(jax.random.fold_in(stream_key, 6), position), (parts,), jnp.float32, least / len(cuts), high / len(cuts))
        return jnp.repeat(jnp.exp(heights), extent[position] // parts).reshape((-1,) + (1,) * (len(extent) - position - 1))

    factor_of = one(*cuts[0])
    for cut in cuts[1:]:
        factor_of = factor_of * one(*cut)
    return factor_of


def gaussian(key, shape, scale, limit, cuts=(), kind=jnp.bfloat16):
    entries = scale * jax.random.normal(key, shape, jnp.float32)
    if cuts:
        entries = entries * level_of(key, shape, cuts, -0.22, 0.18)
    return jnp.clip(entries, -limit, limit).astype(kind)


def setup_inputs(seed: int = 0, part: int = 0) -> dict:
    arg_keys = jax.random.split(jax.random.key(seed), 5)
    part_keys = jax.random.split(jax.random.fold_in(arg_keys[4], part), 5)
    return {
        "activations": gaussian(part_keys[0], (NL, TOKENS, R), 0.3, 1.796875, ((1, 16),)),
        "gradients": gaussian(part_keys[1], (NL, TOKENS, R), 0.3, 1.796875, ((1, 16),)),
        "queries": gaussian(part_keys[2], (Q, TOKENS), TOKENS ** -0.5, 0.125, ((1, 16),)),
        "layer_ids": jax.random.randint(arg_keys[3], (LS,), 0, NL).astype(jnp.int32),
    }


def reference(activations, gradients, queries, layer_ids):
    chosen_inputs = jnp.take(activations, layer_ids, axis=0).astype(jnp.float32)
    chosen_grads = jnp.take(gradients, layer_ids, axis=0).astype(jnp.float32)
    tokens = chosen_inputs.shape[1]
    block_rows = math.gcd(512, tokens)

    def block_of_rows(first_row):
        input_rows = lax.dynamic_slice_in_dim(chosen_inputs, first_row, block_rows, 1)
        grad_rows = lax.dynamic_slice_in_dim(chosen_grads, first_row, block_rows, 1)
        kernel = jnp.zeros((block_rows, tokens), jnp.float32)
        for layer_index in range(LS):
            input_product_matrix = jnp.dot(input_rows[layer_index], chosen_inputs[layer_index].T, precision=lax.Precision.HIGHEST)
            grad_gram = jnp.dot(grad_rows[layer_index], chosen_grads[layer_index].T, precision=lax.Precision.HIGHEST)
            kernel = kernel + input_product_matrix * grad_gram
        second_kernel_function = kernel.astype(jnp.bfloat16)
        return lax.dot_general(queries, second_kernel_function, (((1,), (1,)), ((), ())), preferred_element_type=jnp.float32)

    starts = jnp.arange(tokens // block_rows, dtype=jnp.int32) * block_rows
    pieces = lax.map(block_of_rows, starts)
    return jnp.transpose(pieces, (1, 0, 2)).reshape(queries.shape[0], tokens)
```

```python
import functools

import jax
import jax.numpy as jnp
from jax import lax
from jax.experimental import pallas as pl
from jax.experimental.pallas import tpu as pltpu
from jax.sharding import PartitionSpec as P

VMEM = pltpu.VMEM
NT = (((1,), (1,)), ((), ()))
NN = (((1,), (0,)), ((), ()))


def params(mib):
    return pltpu.CompilerParams(vmem_limit_bytes=mib * 2**20)


def pair_cost(layers, tokens, width, q, pairs):
    return pl.CostEstimate(
        flops=2 * pairs * tokens * tokens * (2 * layers * width + q),
        bytes_accessed=2 * pairs * (2 * layers * tokens + q) * width,
        transcendentals=0,
    )


def vmem_specs(count):
    return [pl.BlockSpec(memory_space=VMEM)] * count


def pack_kernel(ids_ref, acts_ref, grads_ref, queries_ref, out_ref):
    layers, tokens = ids_ref.shape[0], acts_ref.shape[1]
    for l in range(layers):
        i = ids_ref[l]
        out_ref[2 * l * tokens : (2 * l + 1) * tokens] = acts_ref[i]
        out_ref[(2 * l + 1) * tokens : (2 * l + 2) * tokens] = grads_ref[i]
    out_ref[2 * layers * tokens :] = queries_ref[...]


def pack(ids, acts, grads, queries):
    layers, tokens = ids.shape[0], acts.shape[1]
    rows = 2 * layers * tokens + queries.shape[0]
    return pl.pallas_call(
        pack_kernel,
        out_shape=jax.ShapeDtypeStruct((rows, acts.shape[2]), acts.dtype),
        in_specs=[pl.BlockSpec(memory_space=pltpu.SMEM)] + vmem_specs(3),
        out_specs=pl.BlockSpec(memory_space=VMEM),
        compiler_params=params(8),
        name="pack",
    )(ids, acts, grads, queries)


def pair_block(layers, tokens, left, right):
    total = None
    for l in range(layers):
        a = slice(2 * l * tokens, (2 * l + 1) * tokens)
        g = slice((2 * l + 1) * tokens, (2 * l + 2) * tokens)
        x = lax.dot_general(left[a], right[a], NT, preferred_element_type=jnp.float32)
        y = lax.dot_general(left[g], right[g], NT, preferred_element_type=jnp.float32)
        total = x * y if total is None else total + x * y
    return total.astype(jnp.bfloat16)


def near_kernel(layers, tokens, count, *refs):
    own, out = refs[0], refs[count]
    total = None
    for other in refs[:count]:
        k = pair_block(layers, tokens, other, own)
        q = other[2 * layers * tokens :]
        term = lax.dot_general(q, k, NN, preferred_element_type=jnp.float32)
        total = term if total is None else total + term
    out[...] = total


def near(layers, tokens, members):
    q = members[0].shape[0] - 2 * layers * tokens
    return pl.pallas_call(
        functools.partial(near_kernel, layers, tokens, len(members)),
        out_shape=jax.ShapeDtypeStruct((q, tokens), jnp.float32),
        in_specs=vmem_specs(len(members)),
        out_specs=pl.BlockSpec(memory_space=VMEM),
        compiler_params=params(8),
        cost_estimate=pair_cost(layers, tokens, members[0].shape[1], q, len(members)),
        name="near",
    )(*members)


def far_kernel(layers, tokens, count, first, *refs):
    members, visitor = refs[:count], refs[count]
    before = None if first else refs[count + 1 : 2 * count + 1]
    back, parts = refs[-count - 1], refs[-count:]
    visitor_q = visitor[2 * layers * tokens :]
    total = None
    for j in range(count):
        k = pair_block(layers, tokens, members[j], visitor)
        q = members[j][2 * layers * tokens :]
        term = lax.dot_general(q, k, NN, preferred_element_type=jnp.float32)
        total = term if total is None else total + term
        part = lax.dot_general(visitor_q, k, NT, preferred_element_type=jnp.float32)
        parts[j][...] = part if first else before[j][...] + part
    back[...] = total


def far(layers, tokens, members, visitor, before):
    count, q = len(members), visitor.shape[0] - 2 * layers * tokens
    operands = [*members, visitor, *(before or [])]
    outs = pl.pallas_call(
        functools.partial(far_kernel, layers, tokens, count, before is None),
        out_shape=[jax.ShapeDtypeStruct((q, tokens), jnp.float32)] * (count + 1),
        in_specs=vmem_specs(len(operands)),
        out_specs=vmem_specs(count + 1),
        compiler_params=params(8),
        cost_estimate=pair_cost(layers, tokens, visitor.shape[1], 2 * q, count),
        name="far",
    )(*operands)
    return outs[0], list(outs[1:])


def body(acts, grads, queries, ids):
    n = lax.axis_size("tok")
    lanes = next(j for j in (4, 2, 1) if n % j == 0)
    planes = n // lanes
    layers, tokens = ids.shape[0], acts.shape[1]

    def across(x, lane):
        return lax.ppermute(x, "tok", [(i, i ^ lane) for i in range(n)])

    def plane_pairs(shift):
        if 2 * shift < planes:
            return [((p + shift) % planes, p) for p in range(planes)]
        half = [(p, p + shift) for p in range(shift)]
        return [(a, b) if a % 2 == 0 else (b, a) for a, b in half]

    def along(x, pairs):
        route = [(a * lanes + j, b * lanes + j) for a, b in pairs for j in range(lanes)]
        return lax.ppermute(x, "tok", route)

    mine = pack(ids, acts, grads, queries)
    routes = [plane_pairs(s) for s in range(planes // 2, 0, -1)]
    visitors = [along(mine, routes[0])] if routes else []
    members = [mine]
    if lanes > 2:
        members.append(across(mine, 2))
    visitors += [along(mine, r) for r in routes[1:]]
    if lanes > 1:
        members += [across(m, 1) for m in list(members)]
    order = [0, 2, 1, 3][: len(members)] if lanes > 2 else list(range(lanes))

    total = near(layers, tokens, members)
    parts, returned = None, []
    for visitor, route in zip(visitors, routes):
        back, parts = far(layers, tokens, members, visitor, parts)
        returned.append(along(back, [(b, a) for a, b in route]))
    if parts is not None:
        total = total + parts[0]
        for lane, part in list(zip(order, parts))[1:]:
            returned.append(across(part, lane))
    for r in returned:
        total = total + r
    return total


def solution(mesh):
    return jax.shard_map(
        body,
        mesh=mesh,
        in_specs=(
            P(None, ("groups", "tok"), None),
            P(None, ("groups", "tok"), None),
            P(None, ("groups", "tok")),
            P(),
        ),
        out_specs=P(None, ("groups", "tok")),
        check_vma=False,
    )
```

```python
import functools

import jax
import jax.numpy as jnp
from jax import lax
from jax.experimental import pallas as pl
from jax.experimental.pallas import tpu as pltpu
from jax.sharding import PartitionSpec as P

VMEM = pltpu.VMEM
NT = (((1,), (1,)), ((), ()))
NN = (((1,), (0,)), ((), ()))


def params(mib):
    return pltpu.CompilerParams(vmem_limit_bytes=mib * 2**20)


def pair_cost(layers, tokens, width, q, pairs):
    return pl.CostEstimate(
        flops=2 * pairs * tokens * tokens * (2 * layers * width + q),
        bytes_accessed=2 * pairs * (2 * layers * tokens + q) * width,
        transcendentals=0,
    )


def vmem_specs(count):
    return [pl.BlockSpec(memory_space=VMEM)] * count


def pack_kernel(ids_hbm, acts_hbm, grads_hbm, queries_hbm, out_ref, ids, acts, grads, sems):
    layers, tokens = ids.shape[0], acts.shape[1]
    queries = out_ref.at[pl.ds(2 * layers * tokens, queries_hbm.shape[0])]
    moves = [(ids_hbm, ids), (acts_hbm, acts), (grads_hbm, grads), (queries_hbm, queries)]
    copies = [pltpu.make_async_copy(*m, sems.at[i]) for i, m in enumerate(moves)]
    for c in copies:
        c.start()
    for c in copies:
        c.wait()
    for l in range(layers):
        i = ids[l]
        out_ref[2 * l * tokens : (2 * l + 1) * tokens] = acts[i]
        out_ref[(2 * l + 1) * tokens : (2 * l + 2) * tokens] = grads[i]


def pack(ids, acts, grads, queries):
    layers, tokens = ids.shape[0], acts.shape[1]
    rows = 2 * layers * tokens + queries.shape[0]
    held = [pltpu.with_memory_space_constraint(x, pltpu.HBM) for x in (ids, acts, grads, queries)]
    return pl.pallas_call(
        pack_kernel,
        out_shape=jax.ShapeDtypeStruct((rows, acts.shape[2]), acts.dtype),
        in_specs=[pl.BlockSpec(memory_space=pltpu.HBM)] * 4,
        out_specs=pl.BlockSpec(memory_space=VMEM),
        scratch_shapes=[
            pltpu.SMEM(ids.shape, ids.dtype),
            VMEM(acts.shape, acts.dtype),
            VMEM(grads.shape, grads.dtype),
            pltpu.SemaphoreType.DMA((4,)),
        ],
        compiler_params=params(8),
        name="pack",
    )(*held)


def stacked(refs, rows):
    return jnp.concatenate([r[rows] for r in refs], axis=0)


def pair_block(layers, tokens, left, right):
    total = None
    for l in range(layers):
        a = slice(2 * l * tokens, (2 * l + 1) * tokens)
        g = slice((2 * l + 1) * tokens, (2 * l + 2) * tokens)
        x = lax.dot_general(stacked(left, a), stacked(right, a), NT, preferred_element_type=jnp.float32)
        y = lax.dot_general(stacked(left, g), stacked(right, g), NT, preferred_element_type=jnp.float32)
        total = x * y if total is None else total + x * y
    return total.astype(jnp.bfloat16)


def lined(refs, rows):
    return jnp.concatenate([r[rows] for r in refs], axis=1)


def near_kernel(layers, tokens, count, *refs):
    own, out = refs[0], refs[count]
    k = pair_block(layers, tokens, refs[:count], [own])
    q = lined(refs[:count], slice(2 * layers * tokens, own.shape[0]))
    out[...] = lax.dot_general(q, k, NN, preferred_element_type=jnp.float32)


def near(layers, tokens, members):
    q = members[0].shape[0] - 2 * layers * tokens
    return pl.pallas_call(
        functools.partial(near_kernel, layers, tokens, len(members)),
        out_shape=jax.ShapeDtypeStruct((q, tokens), jnp.float32),
        in_specs=vmem_specs(len(members)),
        out_specs=pl.BlockSpec(memory_space=VMEM),
        compiler_params=params(8),
        cost_estimate=pair_cost(layers, tokens, members[0].shape[1], q, len(members)),
        name="near",
    )(*members)


def far_kernel(layers, tokens, count, first, *refs):
    members, visitor = refs[:count], refs[count]
    before = None if first else refs[count + 1 : 2 * count + 1]
    back, parts = refs[-count - 1], refs[-count:]
    tail = slice(2 * layers * tokens, visitor.shape[0])
    k = pair_block(layers, tokens, members, [visitor])
    back[...] = lax.dot_general(lined(members, tail), k, NN, preferred_element_type=jnp.float32)
    every = lax.dot_general(visitor[tail], k, NT, preferred_element_type=jnp.float32)
    for j in range(count):
        part = every[:, j * tokens : (j + 1) * tokens]
        parts[j][...] = part if first else before[j][...] + part


def far(layers, tokens, members, visitor, before):
    count, q = len(members), visitor.shape[0] - 2 * layers * tokens
    operands = [*members, visitor, *(before or [])]
    outs = pl.pallas_call(
        functools.partial(far_kernel, layers, tokens, count, before is None),
        out_shape=[jax.ShapeDtypeStruct((q, tokens), jnp.float32)] * (count + 1),
        in_specs=vmem_specs(len(operands)),
        out_specs=vmem_specs(count + 1),
        compiler_params=params(8),
        cost_estimate=pair_cost(layers, tokens, visitor.shape[1], 2 * q, count),
        name="far",
    )(*operands)
    return outs[0], list(outs[1:])


def split(n):
    lanes = next(j for j in (4, 2, 1) if n % j == 0)
    planes = n // lanes
    routes = []
    for shift in range(planes // 2, 0, -1):
        if 2 * shift < planes:
            routes.append([(p, (p + shift) % planes) for p in range(planes)])
        else:
            half = [(p, p + shift) for p in range(shift)]
            routes.append([(a, b) if a % 2 == 0 else (b, a) for a, b in half])
    return lanes, routes


def body(acts, grads, queries, ids):
    n = lax.axis_size("tok")
    lanes, routes = split(n)
    layers, tokens = ids.shape[0], acts.shape[1]

    def across(x, lane):
        return lax.ppermute(x, "tok", [(i, i ^ lane) for i in range(n)])

    def along(x, pairs):
        route = [(a * lanes + j, b * lanes + j) for a, b in pairs for j in range(lanes)]
        return lax.ppermute(x, "tok", route)

    mine = pack(ids, acts, grads, queries)
    visitors = [along(mine, r) for r in routes]
    members = [mine]
    if lanes > 1:
        members.append(across(mine, 1))
    if lanes > 2:
        other = across(mine, 2)
        members += [other, across(other, 1)]

    total = near(layers, tokens, members)
    parts, returned = None, []
    for visitor, route in zip(visitors, routes):
        back, parts = far(layers, tokens, members, visitor, parts)
        returned.append(along(back, [(b, a) for a, b in route]))
    if parts is None:
        return total
    if lanes == 1:
        total = total + parts[0]
    elif lanes == 2:
        total = total + parts[0]
        returned.append(across(parts[1], 1))
    else:
        total = total + parts[0]
        returned += [across(parts[j], k) for j, k in ((2, 2), (3, 3), (1, 1))]
    for r in returned:
        total = total + r
    return total


def solution(mesh):
    return jax.shard_map(
        body,
        mesh=mesh,
        in_specs=(
            P(None, ("groups", "tok"), None),
            P(None, ("groups", "tok"), None),
            P(None, ("groups", "tok")),
            P(),
        ),
        out_specs=P(None, ("groups", "tok")),
        check_vma=False,
    )
```

```python
import functools

import jax
import jax.numpy as jnp
from jax import lax
from jax.experimental import pallas as pl
from jax.experimental.pallas import tpu as pltpu
from jax.sharding import PartitionSpec as P

VMEM = pltpu.VMEM
NT = (((1,), (1,)), ((), ()))
NN = (((1,), (0,)), ((), ()))


def params(mib):
    return pltpu.CompilerParams(vmem_limit_bytes=mib * 2**20)


def pair_cost(layers, tokens, width, q, pairs):
    return pl.CostEstimate(
        flops=2 * pairs * tokens * tokens * (2 * layers * width + q),
        bytes_accessed=2 * pairs * (2 * layers * tokens + q) * width,
        transcendentals=0,
    )


def vmem_specs(count):
    return [pl.BlockSpec(memory_space=VMEM)] * count


def pack_kernel(ids_hbm, acts_hbm, grads_hbm, queries_hbm, out_ref, ids, acts, grads, sems):
    layers, tokens = ids.shape[0], acts.shape[1]
    queries = out_ref.at[pl.ds(2 * layers * tokens, queries_hbm.shape[0])]
    moves = [(ids_hbm, ids), (acts_hbm, acts), (grads_hbm, grads), (queries_hbm, queries)]
    copies = [pltpu.make_async_copy(*m, sems.at[i]) for i, m in enumerate(moves)]
    for c in copies:
        c.start()
    for c in copies:
        c.wait()
    for l in range(layers):
        i = ids[l]
        out_ref[2 * l * tokens : (2 * l + 1) * tokens] = acts[i]
        out_ref[(2 * l + 1) * tokens : (2 * l + 2) * tokens] = grads[i]


def pack(ids, acts, grads, queries):
    layers, tokens = ids.shape[0], acts.shape[1]
    rows = 2 * layers * tokens + queries.shape[0]
    held = [pltpu.with_memory_space_constraint(x, pltpu.HBM) for x in (ids, acts, grads, queries)]
    return pl.pallas_call(
        pack_kernel,
        out_shape=jax.ShapeDtypeStruct((rows, acts.shape[2]), acts.dtype),
        in_specs=[pl.BlockSpec(memory_space=pltpu.HBM)] * 4,
        out_specs=pl.BlockSpec(memory_space=VMEM),
        scratch_shapes=[
            pltpu.SMEM(ids.shape, ids.dtype),
            VMEM(acts.shape, acts.dtype),
            VMEM(grads.shape, grads.dtype),
            pltpu.SemaphoreType.DMA((4,)),
        ],
        compiler_params=params(8),
        name="pack",
    )(*held)


def stacked(refs, rows):
    return jnp.concatenate([r[rows] for r in refs], axis=0)


def pair_block(layers, tokens, left, right):
    total = None
    for l in range(layers):
        a = slice(2 * l * tokens, (2 * l + 1) * tokens)
        g = slice((2 * l + 1) * tokens, (2 * l + 2) * tokens)
        x = lax.dot_general(stacked(left, a), stacked(right, a), NT, preferred_element_type=jnp.float32)
        y = lax.dot_general(stacked(left, g), stacked(right, g), NT, preferred_element_type=jnp.float32)
        total = x * y if total is None else total + x * y
    return total.astype(jnp.bfloat16)


def lined(refs, rows):
    return jnp.concatenate([r[rows] for r in refs], axis=1)


def near_kernel(layers, tokens, count, *refs):
    own, out = refs[0], refs[count]
    k = pair_block(layers, tokens, refs[:count], [own])
    q = lined(refs[:count], slice(2 * layers * tokens, own.shape[0]))
    out[...] = lax.dot_general(q, k, NN, preferred_element_type=jnp.float32)


def near(layers, tokens, members):
    q = members[0].shape[0] - 2 * layers * tokens
    return pl.pallas_call(
        functools.partial(near_kernel, layers, tokens, len(members)),
        out_shape=jax.ShapeDtypeStruct((q, tokens), jnp.float32),
        in_specs=vmem_specs(len(members)),
        out_specs=pl.BlockSpec(memory_space=VMEM),
        compiler_params=params(8),
        cost_estimate=pair_cost(layers, tokens, members[0].shape[1], q, len(members)),
        name="near",
    )(*members)


def far_kernel(layers, tokens, count, first, *refs):
    members, visitor = refs[:count], refs[count]
    before = None if first else refs[count + 1 : 2 * count + 1]
    back, parts = refs[-count - 1], refs[-count:]
    tail = slice(2 * layers * tokens, visitor.shape[0])
    k = pair_block(layers, tokens, members, [visitor])
    back[...] = lax.dot_general(lined(members, tail), k, NN, preferred_element_type=jnp.float32)
    every = lax.dot_general(visitor[tail], k, NT, preferred_element_type=jnp.float32)
    for j in range(count):
        part = every[:, j * tokens : (j + 1) * tokens]
        parts[j][...] = part if first else before[j][...] + part


def far(layers, tokens, members, visitor, before):
    count, q = len(members), visitor.shape[0] - 2 * layers * tokens
    operands = [*members, visitor, *(before or [])]
    outs = pl.pallas_call(
        functools.partial(far_kernel, layers, tokens, count, before is None),
        out_shape=[jax.ShapeDtypeStruct((q, tokens), jnp.float32)] * (count + 1),
        in_specs=vmem_specs(len(operands)),
        out_specs=vmem_specs(count + 1),
        compiler_params=params(8),
        cost_estimate=pair_cost(layers, tokens, visitor.shape[1], 2 * q, count),
        name="far",
    )(*operands)
    return outs[0], list(outs[1:])


def split(n):
    lanes = next(j for j in (4, 2, 1) if n % j == 0)
    planes = n // lanes
    routes = []
    for shift in range(1, planes // 2 + 1):
        if 2 * shift < planes:
            routes.append([(p, (p + shift) % planes) for p in range(planes)])
        else:
            half = [(p, p + shift) for p in range(shift)]
            routes.append([(a, b) if a % 2 == 0 else (b, a) for a, b in half])
    return lanes, routes


def body(acts, grads, queries, ids):
    n = lax.axis_size("tok")
    lanes, routes = split(n)
    layers, tokens = ids.shape[0], acts.shape[1]

    def across(x, lane):
        return lax.ppermute(x, "tok", [(i, i ^ lane) for i in range(n)])

    def along(x, pairs):
        route = [(a * lanes + j, b * lanes + j) for a, b in pairs for j in range(lanes)]
        return lax.ppermute(x, "tok", route)

    mine = pack(ids, acts, grads, queries)
    visitors = [along(mine, r) for r in routes]
    members = [mine]
    if lanes > 1:
        members.append(across(mine, 1))
    if lanes > 2:
        other = across(mine, 2)
        members += [other, across(other, 1)]

    total = near(layers, tokens, members)
    parts, returned = None, []
    for visitor, route in zip(visitors, routes):
        back, parts = far(layers, tokens, members, visitor, parts)
        returned.append(along(back, [(b, a) for a, b in route]))
    if parts is None:
        return total
    if lanes == 1:
        total = total + parts[0]
    elif lanes == 2:
        total = total + parts[0]
        returned.append(across(parts[1], 1))
    else:
        met = across(jnp.stack([parts[1], parts[3]]), 1)
        total = total + parts[0] + met[0]
        returned.append(across(parts[2] + met[1], 2))
    for r in returned:
        total = total + r
    return total


def solution(mesh):
    return jax.shard_map(
        body,
        mesh=mesh,
        in_specs=(
            P(None, ("groups", "tok"), None),
            P(None, ("groups", "tok"), None),
            P(None, ("groups", "tok")),
            P(),
        ),
        out_specs=P(None, ("groups", "tok")),
        check_vma=False,
    )
```

```python
import functools

import jax
import jax.numpy as jnp
from jax import lax
from jax.experimental import pallas as pl
from jax.experimental.pallas import tpu as pltpu
from jax.sharding import PartitionSpec as P

VMEM = pltpu.VMEM
NT = (((1,), (1,)), ((), ()))
NN = (((1,), (0,)), ((), ()))


def params(mib):
    return pltpu.CompilerParams(vmem_limit_bytes=mib * 2**20)


def pair_cost(layers, tokens, width, q, pairs):
    return pl.CostEstimate(
        flops=2 * pairs * tokens * tokens * (2 * layers * width + q),
        bytes_accessed=2 * pairs * (2 * layers * tokens + q) * width,
        transcendentals=0,
    )


def vmem_specs(count):
    return [pl.BlockSpec(memory_space=VMEM)] * count


def pack_kernel(ids_hbm, acts_hbm, grads_hbm, queries_hbm, out_ref, ids, acts, grads, sems):
    layers, tokens = ids.shape[0], acts.shape[1]
    queries = out_ref.at[pl.ds(2 * layers * tokens, queries_hbm.shape[0])]
    moves = [(ids_hbm, ids), (acts_hbm, acts), (grads_hbm, grads), (queries_hbm, queries)]
    copies = [pltpu.make_async_copy(*m, sems.at[i]) for i, m in enumerate(moves)]
    for c in copies:
        c.start()
    for c in copies:
        c.wait()
    for l in range(layers):
        i = ids[l]
        out_ref[2 * l * tokens : (2 * l + 1) * tokens] = acts[i]
        out_ref[(2 * l + 1) * tokens : (2 * l + 2) * tokens] = grads[i]


def pack(ids, acts, grads, queries):
    layers, tokens = ids.shape[0], acts.shape[1]
    rows = 2 * layers * tokens + queries.shape[0]
    held = [pltpu.with_memory_space_constraint(x, pltpu.HBM) for x in (ids, acts, grads, queries)]
    return pl.pallas_call(
        pack_kernel,
        out_shape=jax.ShapeDtypeStruct((rows, acts.shape[2]), acts.dtype),
        in_specs=[pl.BlockSpec(memory_space=pltpu.HBM)] * 4,
        out_specs=pl.BlockSpec(memory_space=VMEM),
        scratch_shapes=[
            pltpu.SMEM(ids.shape, ids.dtype),
            VMEM(acts.shape, acts.dtype),
            VMEM(grads.shape, grads.dtype),
            pltpu.SemaphoreType.DMA((4,)),
        ],
        compiler_params=params(8),
        name="pack",
    )(*held)


def stacked(refs, rows):
    return jnp.concatenate([r[rows] for r in refs], axis=0)


def pair_block(layers, tokens, left, right):
    total = None
    for l in range(layers):
        a = slice(2 * l * tokens, (2 * l + 1) * tokens)
        g = slice((2 * l + 1) * tokens, (2 * l + 2) * tokens)
        x = lax.dot_general(stacked(left, a), stacked(right, a), NT, preferred_element_type=jnp.float32)
        y = lax.dot_general(stacked(left, g), stacked(right, g), NT, preferred_element_type=jnp.float32)
        total = x * y if total is None else total + x * y
    return total.astype(jnp.bfloat16)


def lined(refs, rows):
    return jnp.concatenate([r[rows] for r in refs], axis=1)


def near_kernel(layers, tokens, count, *refs):
    own, out = refs[0], refs[count]
    k = pair_block(layers, tokens, refs[:count], [own])
    q = lined(refs[:count], slice(2 * layers * tokens, own.shape[0]))
    out[...] = lax.dot_general(q, k, NN, preferred_element_type=jnp.float32)


def near(layers, tokens, members):
    q = members[0].shape[0] - 2 * layers * tokens
    return pl.pallas_call(
        functools.partial(near_kernel, layers, tokens, len(members)),
        out_shape=jax.ShapeDtypeStruct((q, tokens), jnp.float32),
        in_specs=vmem_specs(len(members)),
        out_specs=pl.BlockSpec(memory_space=VMEM),
        compiler_params=params(8),
        cost_estimate=pair_cost(layers, tokens, members[0].shape[1], q, len(members)),
        name="near",
    )(*members)


def far_kernel(layers, tokens, count, first, *refs):
    members, visitor = refs[:count], refs[count]
    before = None if first else refs[count + 1 : 2 * count + 1]
    back, parts = refs[-count - 1], refs[-count:]
    tail = slice(2 * layers * tokens, visitor.shape[0])
    k = pair_block(layers, tokens, members, [visitor])
    back[...] = lax.dot_general(lined(members, tail), k, NN, preferred_element_type=jnp.float32)
    every = lax.dot_general(visitor[tail], k, NT, preferred_element_type=jnp.float32)
    for j in range(count):
        part = every[:, j * tokens : (j + 1) * tokens]
        parts[j][...] = part if first else before[j][...] + part


def far(layers, tokens, members, visitor, before):
    count, q = len(members), visitor.shape[0] - 2 * layers * tokens
    operands = [*members, visitor, *(before or [])]
    outs = pl.pallas_call(
        functools.partial(far_kernel, layers, tokens, count, before is None),
        out_shape=[jax.ShapeDtypeStruct((q, tokens), jnp.float32)] * (count + 1),
        in_specs=vmem_specs(len(operands)),
        out_specs=vmem_specs(count + 1),
        compiler_params=params(8),
        cost_estimate=pair_cost(layers, tokens, visitor.shape[1], 2 * q, count),
        name="far",
    )(*operands)
    return outs[0], list(outs[1:])


def split(n):
    lanes = next(j for j in (4, 2, 1) if n % j == 0)
    planes = n // lanes
    routes = []
    for shift in range(1, planes // 2 + 1):
        if 2 * shift < planes:
            routes.append([(p, (p + shift) % planes) for p in range(planes)])
        else:
            half = [(p, p + shift) for p in range(shift)]
            routes.append([(a, b) if a % 2 == 0 else (b, a) for a, b in half])
    return lanes, routes


def filled(pairs, planes):
    idle = [p for p in range(planes) if p not in [a for a, _ in pairs]]
    bare = [p for p in range(planes) if p not in [b for _, b in pairs]]
    return pairs + list(zip(idle, bare))


def body(acts, grads, queries, ids):
    n = lax.axis_size("tok")
    lanes, routes = split(n)
    planes = n // lanes
    layers, tokens = ids.shape[0], acts.shape[1]

    def across(x, lane):
        return lax.ppermute(x, "tok", [(i, i ^ lane) for i in range(n)])

    def along(x, pairs):
        flip = min(1, lanes - 1)
        route = [(a * lanes + j, b * lanes + (j ^ flip)) for a, b in pairs for j in range(lanes)]
        return lax.ppermute(x, "tok", route)

    mine = pack(ids, acts, grads, queries)
    visitors = [along(mine, r) for r in routes]
    members = [mine]
    if lanes > 1:
        members.append(across(mine, 1))
    if lanes > 2:
        other = across(mine, 2)
        members += [other, across(other, 1)]

    total = near(layers, tokens, members)
    parts, returned = None, []
    for visitor, route in zip(visitors, routes):
        back, parts = far(layers, tokens, members, visitor, parts)
        returned.append(along(back, filled([(b, a) for a, b in route], planes)))
    if parts is None:
        return total
    if lanes == 1:
        total = total + parts[0]
    elif lanes == 2:
        total = total + parts[0]
        returned.append(across(parts[1], 1))
    else:
        met = across(jnp.stack([parts[1], parts[3]]), 1)
        total = total + parts[0] + met[0]
        returned.append(across(parts[2] + met[1], 2))
    for r in returned:
        total = total + r
    return total


def solution(mesh):
    return jax.shard_map(
        body,
        mesh=mesh,
        in_specs=(
            P(None, ("groups", "tok"), None),
            P(None, ("groups", "tok"), None),
            P(None, ("groups", "tok")),
            P(),
        ),
        out_specs=P(None, ("groups", "tok")),
        check_vma=False,
    )
```
